32 devices in a mesh: horizon: 8 (over z, x), batch: 4 (over y, core).
Axes of the slice: x: 2, y: 2, z: 4, core: 2. Of those that a mesh axis runs over, the one named last changes fastest.
Arguments:
- dynamics: float32 [4, 64, 48, 48], P('batch', 'horizon'), may hold values from -0.1 to 1.1
- inputs: float32 [4, 64, 48, 16], P('batch', 'horizon'), may hold values from -0.6 to 0.6
- state_cost: float32 [4, 64, 48, 48], P('batch', 'horizon'), may hold values from -1 to 1, as said below
- input_cost: float32 [4, 64, 16, 16], P('batch', 'horizon'), may hold values from -0.2 to 2.2, as said below
- drift: float32 [4, 64, 48], P('batch', 'horizon'), may hold values from -0.6 to 0.6
- target: float32 [4, 64, 48], P('batch', 'horizon'), may hold values from -6 to 6
- initial: float32 [4, 48], P('batch'), may hold values from -6 to 6
Outputs:
- hessian: float32 [4, 1024, 1024], P('batch', 'horizon')
- gradient: float32 [4, 1024], P('batch', 'horizon')
The draws below stay inside these ranges and needn't reach their ends.
Inputs may be any that keep to these rules, and one draw needn't show every extreme that they name: `state_cost`: each 48 x 48 matrix is symmetric and positive definite. `input_cost`: each 16 x 16 matrix is symmetric and positive definite.
All inputs are finite; a program needn't handle non-finite values.
Results may differ from the reference program's by a relative error of at most 0.0003.
Values sent between devices are 32-bit elements; how exact they have to be, the bound alone decides.
No kernel may reach another device: no remote copies, remote signals or barrier semaphores. Data moves between devices by JAX's collectives and lax.ppermute only.
A program may use at most 128 MiB of HBM per device.

```python
import math
import jax
import jax.numpy as jnp
from jax import lax

NX = 48
NU = 16
INTERVAL_TOTAL = 64
TASK_TOTAL = 4


def draw_dynamics(key, part):
    seed_handles = jax.random.split(jax.random.fold_in(key, 11), 4)
    lowest, highest = (0.5, 12.0)
    expansion_speed = jnp.exp(jax.random.uniform(seed_handles[0], (TASK_TOTAL, 1, NX), jnp.float32, math.log(lowest), math.log(highest))) / INTERVAL_TOTAL
    dispersion_span = jnp.exp(jax.random.uniform(seed_handles[1], (TASK_TOTAL, INTERVAL_TOTAL, NX), jnp.float32, math.log(0.5), math.log(2.0)))
    spike_magnitude = jnp.where(jax.random.uniform(seed_handles[2], (TASK_TOTAL, INTERVAL_TOTAL, 1), jnp.float32) < 4.0 / INTERVAL_TOTAL, 0.6, 1.0)
    damping_multiplier = jnp.exp(-expansion_speed * dispersion_span) * spike_magnitude
    noise = jnp.clip(jax.random.normal(seed_handles[3], (TASK_TOTAL, INTERVAL_TOTAL, NX, NX), jnp.float32), -4.0, 4.0) * (0.2 / NX)
    return noise + damping_multiplier[..., None] * jnp.eye(NX, dtype=jnp.float32)


def draw_state_cost(key, part):
    seed_handles = jax.random.split(jax.random.fold_in(key, 23), 2)
    lowest, highest = (2.0, 20.0)
    divisor = float(max(INTERVAL_TOTAL, 48))
    diagonal = jnp.exp(jax.random.uniform(seed_handles[0], (TASK_TOTAL, INTERVAL_TOTAL, NX), jnp.float32, math.log(lowest), math.log(highest))) / divisor
    raw = jnp.clip(jax.random.normal(seed_handles[1], (TASK_TOTAL, INTERVAL_TOTAL, NX, NX), jnp.float32), -4.0, 4.0) * (0.1 / divisor)
    symmetric = (raw + jnp.swapaxes(raw, -1, -2)) * 0.7071
    return symmetric + diagonal[..., None] * jnp.eye(NX, dtype=jnp.float32)


def draw_input_cost(key, part):
    seed_handles = jax.random.split(jax.random.fold_in(key, 37), 2)
    diagonal = jnp.exp(jax.random.uniform(seed_handles[0], (TASK_TOTAL, INTERVAL_TOTAL, NU), jnp.float32, math.log(0.5), math.log(2.0)))
    raw = jnp.clip(jax.random.normal(seed_handles[1], (TASK_TOTAL, INTERVAL_TOTAL, NU, NU), jnp.float32), -4.0, 4.0) * 0.03
    symmetric = (raw + jnp.swapaxes(raw, -1, -2)) * 0.7071
    return symmetric + diagonal[..., None] * jnp.eye(NU, dtype=jnp.float32)


def steps_of(rng, dims, shards, least, largest):
    gain = 1.0
    for axis_at, blocks in shards:
        heights = jax.random.uniform(jax.random.fold_in(jax.random.fold_in(rng, 6), axis_at), (blocks,), jnp.float32, least / len(shards), largest / len(shards))
        gain = gain * jnp.repeat(jnp.exp(heights), dims[axis_at] // blocks).reshape((-1,) + (1,) * (len(dims) - 1 - axis_at))
    return gain


def centred(stream_key, shape, scale, bound, pieces=(), kind=jnp.bfloat16):
    values = scale * jax.random.normal(stream_key, shape, jnp.float32)
    if pieces:
        values = values * steps_of(stream_key, shape, pieces, -0.22, 0.18)
    return jnp.clip(values, -bound, bound).astype(kind)


def setup_inputs(seed: int = 0) -> dict:
    arg_keys = jax.random.split(jax.random.key(seed), 8)
    return {
        "dynamics": draw_dynamics(jax.random.fold_in(arg_keys[7], 71), 0),
        "inputs": centred(arg_keys[1], (TASK_TOTAL, INTERVAL_TOTAL, NX, NU), 0.1, 0.6, ((0, 4), (1, 8)), jnp.float32),
        "state_cost": draw_state_cost(jax.random.fold_in(arg_keys[7], 71), 0),
        "input_cost": draw_input_cost(jax.random.fold_in(arg_keys[7], 71), 0),
        "drift": centred(arg_keys[4], (TASK_TOTAL, INTERVAL_TOTAL, NX), 0.1, 0.6, ((0, 4), (1, 8)), jnp.float32),
        "target": centred(arg_keys[5], (TASK_TOTAL, INTERVAL_TOTAL, NX), 1.0, 6.0, ((0, 4), (1, 8)), jnp.float32),
        "initial": centred(arg_keys[6], (TASK_TOTAL, NX), 1.0, 6.0, ((0, 4),), jnp.float32),
    }


HI = lax.Precision.HIGHEST


def condense_one(items):
    section_dynamics, section_inputs, section_costs, section_input_costs, section_drift, section_target, start = items
    width = INTERVAL_TOTAL * NU

    def roll_states(state, parts):
        matrix, shift_vec, goal, weight = parts
        after = jnp.dot(matrix, state, precision=HI) + shift_vec
        return after, jnp.dot(weight, after - goal, precision=HI)

    _, weighted = lax.scan(roll_states, start, (section_dynamics, section_drift, section_target, section_costs))

    def sweep_costs(tail, parts):
        matrix, weight = parts
        total_cost = weight + tail
        return jnp.dot(matrix.T, jnp.dot(total_cost, matrix, precision=HI), precision=HI), total_cost

    _, cost_to_go = lax.scan(sweep_costs, jnp.zeros((NX, NX), jnp.float32), (section_dynamics, section_costs), reverse=True)
    values = jnp.einsum("sij,sjk->sik", cost_to_go, section_inputs, precision=HI)

    def sweep_columns(carry, parts):
        block, vector = carry
        matrix, control, value, weight, index = parts
        row_block = jnp.dot(control.T, block, precision=HI)
        summed = weight + vector
        grad_block = jnp.dot(control.T, summed, precision=HI)
        placed = lax.dynamic_update_slice_in_dim(block, value, (index * NU).astype(jnp.int32), 1)
        return (jnp.dot(matrix.T, placed, precision=HI), jnp.dot(matrix.T, summed, precision=HI)), (row_block, grad_block)

    indices = jnp.arange(INTERVAL_TOTAL, dtype=jnp.int32)
    start_carry = (jnp.zeros((NX, width), jnp.float32), jnp.zeros((NX,), jnp.float32))
    _, (row_blocks, grad_blocks) = lax.scan(sweep_columns, start_carry, (section_dynamics, section_inputs, values, weighted, indices), reverse=True)
    upper = row_blocks.reshape(width, width)
    diagonal_blocks = jnp.einsum("sji,sjk->sik", section_inputs, values, precision=HI) + section_input_costs
    block_diag = jnp.einsum("st,sij->sitj", jnp.eye(INTERVAL_TOTAL, dtype=jnp.float32), diagonal_blocks, precision=HI).reshape(width, width)
    return upper + upper.T + block_diag, grad_blocks.reshape(width)


def reference(dynamics, inputs, state_cost, input_cost, drift, target, initial):
    hessian, gradient = lax.map(condense_one, (dynamics, inputs, state_cost, input_cost, drift, target, initial))
    return (hessian, gradient)
```

```python
import functools

import jax
import jax.numpy as jnp
from jax import lax
from jax.experimental import pallas as pl
from jax.experimental.pallas import tpu as pltpu
from jax.sharding import PartitionSpec as P

LANES = 128
HALF = 64


def split(x):
    high = x.astype(jnp.bfloat16)
    return high, (x - high.astype(jnp.float32)).astype(jnp.bfloat16)


def product(left, right, trans=False):
    dims = (((0 if trans else 1,), (0,)), ((), ()))
    mul = functools.partial(
        lax.dot_general, dimension_numbers=dims, preferred_element_type=jnp.float32
    )
    (lh, ll), (rh, rl) = split(left), split(right)
    return mul(lh, rh) + (mul(lh, rl) + mul(ll, rh))


def iota(shape, dim):
    return lax.broadcasted_iota(jnp.int32, shape, dim)


def spread(blocks, rows_of):
    total, n = blocks.shape
    width = total // rows_of * n
    copies = (iota((n, width), 1) % n == iota((n, width), 0)).astype(jnp.float32)
    wide = product(blocks, copies)
    shape = (total, width)
    return jnp.where(iota(shape, 0) // rows_of == iota(shape, 1) // n, wide, 0.0)


def respond(first, last, start):
    if last - first == 1:
        return [start[first]]
    middle = (first + last) // 2
    left, right = respond(first, middle, start), respond(middle, last, start)
    nx = left[0].shape[0]
    cols = left[0].shape[1]
    maps = [x[:, cols - LANES : cols - LANES + nx] for x in right]
    through = product(jnp.concatenate(maps, 0), left[-1])
    keep = (iota((nx, cols), 1) < cols - LANES) | (iota((nx, cols), 1) >= cols - LANES + nx)
    return left + [
        through[i * nx : (i + 1) * nx] + jnp.where(keep, x, 0.0) for i, x in enumerate(right)
    ]


def local_kernel(a_ref, b_ref, q_ref, r_ref, f_ref, g_ref, pay_ref, own_ref, row_ref):
    problems, sections, nx, nu = b_ref.shape
    cols = sections * nu
    for p in range(problems):
        placed = spread(jnp.concatenate([b_ref[p, s] for s in range(sections)], 0), nx)
        drift = f_ref[p].T
        target = g_ref[p].T
        pad = jnp.zeros((nx, LANES - nx - 1), jnp.float32)
        start = [
            jnp.concatenate(
                [
                    placed[s * nx : (s + 1) * nx],
                    jnp.concatenate([a_ref[p, s], drift[:, s : s + 1], pad], 1),
                ],
                1,
            )
            for s in range(sections)
        ]
        states = respond(0, sections, start)
        lane = iota((nx, cols + LANES), 1)
        errors = [
            jnp.where(lane == cols + nx, x - target[:, s : s + 1], x)
            for s, x in enumerate(states)
        ]
        weighted = [product(q_ref[p, s], e) for s, e in enumerate(errors)]
        square = product(
            jnp.concatenate(errors, 0), jnp.concatenate(weighted, 0), trans=True
        )
        own_ref[p] = square[:cols, :cols] + spread(
            r_ref[p].reshape(sections * nu, nu), nu
        )
        row_ref[p] = square[cols + nx : cols + nx + 1, :cols]
        end = states[-1]
        pay_ref[p, :, :cols] = square[cols : cols + nx, :cols]
        pay_ref[p, :, cols : 2 * cols] = end[:, :cols]
        pay_ref[p, :, 2 * cols :] = jnp.concatenate(
            [end[:, cols : cols + HALF], square[cols : cols + nx, cols : cols + HALF]], 1
        )


def join_kernel(count, *refs):
    pays, (own_ref, row_ref, x_ref, h_ref, grad_ref) = refs[:count], refs[count:]
    device = lax.axis_index("horizon")
    problems, cols, _ = own_ref.shape
    nx = x_ref.shape[-1]
    for p in range(problems):
        gain = lambda k: pays[k][p, :, :cols]
        reach = lambda k: pays[k][p, :, cols : 2 * cols]
        maps = [pays[k][p, :, 2 * cols : 2 * cols + HALF] for k in range(count)]
        costs = [pays[k][p, :, 2 * cols + HALF :] for k in range(count)]
        upper = [device + k < count for k in range(count)]
        moved = [None, reach(0)]
        for k in range(1, count):
            moved[k] = jnp.where(upper[k], moved[k], 0.0)
            if k + 1 < count:
                moved.append(product(maps[k][:, :nx], moved[k]))
        last = iota((HALF, cols), 0) >= nx
        costate = jnp.zeros((HALF, cols), jnp.float32)
        above = [None] * count
        for k in reversed(range(1, count)):
            above[k] = costate[:nx]
            costate = (
                product(costs[k], moved[k], True)
                + product(maps[k], costate[:nx], True)
                + jnp.where(last, costate, 0.0)
            )
        own_at = pl.multiple_of(device * cols, cols)
        h_ref[p, :, pl.ds(own_at, cols)] = own_ref[p] + product(costate[:nx], reach(0), True)
        pad = jnp.zeros((HALF - nx - 1, cols), jnp.float32)
        costate = (
            jnp.concatenate([gain(0), row_ref[p], pad], 0)
            + product(maps[0], costate[:nx], True)
            + jnp.where(last, costate, 0.0)
        )
        for k in reversed(range(1, count)):
            at = pl.multiple_of(lax.rem(device + k, count) * cols, cols)
            left = jnp.concatenate(
                [moved[k], jnp.where(upper[k], above[k], costate[:nx])], 0
            )
            right = jnp.concatenate([gain(k), reach(k)], 0)
            h_ref[p, :, pl.ds(at, cols)] = product(left, right, True)
            costate = jnp.where(
                upper[k],
                costate,
                product(maps[k], costate[:nx], True) + jnp.where(last, costate, 0.0),
            )
        grad_ref[pl.ds(p, 1), :] = product(x_ref[pl.ds(p, 1), :], costate[:nx]) + costate[nx : nx + 1]


def body(dynamics, inputs, state_cost, input_cost, drift, target, initial):
    count = lax.axis_size("horizon")
    problems, sections, nx, nu = inputs.shape
    cols = sections * nu
    f32 = jnp.float32
    pay, own, row = pl.pallas_call(
        local_kernel,
        out_shape=(
            jax.ShapeDtypeStruct((problems, nx, 2 * cols + LANES), f32),
            jax.ShapeDtypeStruct((problems, cols, cols), f32),
            jax.ShapeDtypeStruct((problems, 1, cols), f32),
        ),
        name="local",
    )(dynamics, inputs, state_cost, input_cost, drift, target)
    pays = [pay] + [
        lax.ppermute(pay, "horizon", [((i + k) % count, i) for i in range(count)])
        for k in range(1, count)
    ]
    return pl.pallas_call(
        functools.partial(join_kernel, count),
        out_shape=(
            jax.ShapeDtypeStruct((problems, cols, count * cols), f32),
            jax.ShapeDtypeStruct((problems, cols), f32),
        ),
        name="join",
    )(*pays, own, row, initial)


def solution(mesh):
    in_specs = (
        P("batch", "horizon", None, None),
        P("batch", "horizon", None, None),
        P("batch", "horizon", None, None),
        P("batch", "horizon", None, None),
        P("batch", "horizon", None),
        P("batch", "horizon", None),
        P("batch", None),
    )
    out_specs = (P("batch", "horizon", None), P("batch", "horizon"))
    return jax.shard_map(body, mesh=mesh, in_specs=in_specs, out_specs=out_specs, check_vma=False)
```

```python
import functools

import jax
import jax.numpy as jnp
from jax import lax
from jax.experimental import pallas as pl
from jax.experimental.pallas import tpu as pltpu
from jax.sharding import PartitionSpec as P

LANES = 128
HALF = 64


def split(x):
    high = x.astype(jnp.bfloat16)
    return high, (x - high.astype(jnp.float32)).astype(jnp.bfloat16)


def product(left, right, form="nn"):
    dims = (((0 if form[0] == "t" else 1,), (1 if form[1] == "t" else 0,)), ((), ()))
    mul = functools.partial(
        lax.dot_general, dimension_numbers=dims, preferred_element_type=jnp.float32
    )
    (lh, ll), (rh, rl) = split(left), split(right)
    return mul(lh, rh) + (mul(lh, rl) + mul(ll, rh))


def iota(shape, dim):
    return lax.broadcasted_iota(jnp.int32, shape, dim)


def respond(first, last, start):
    if last - first == 1:
        return [start[first]]
    middle = (first + last) // 2
    left, right = respond(first, middle, start), respond(middle, last, start)
    nx, width = left[0].shape
    cols = width - LANES
    maps = [x[:, cols : cols + nx] for x in right]
    through = product(jnp.concatenate(maps, 0), left[-1])
    lane = iota((nx, width), 1)
    keep = (lane < cols) | (lane >= cols + nx)
    return left + [
        through[i * nx : (i + 1) * nx] + jnp.where(keep, x, 0.0) for i, x in enumerate(right)
    ]


def local_kernel(*refs):
    sources, (pay_ref, own_ref, side_ref, state_ref) = refs[:7], refs[7:11]
    held, sem = refs[11:18], refs[18]
    copies = [
        pltpu.make_async_copy(source, target, sem.at[i])
        for i, (source, target) in enumerate(zip(sources, held))
    ]
    for copy in copies:
        copy.start()
    for copy in copies:
        copy.wait()
    a_ref, b_ref, f_ref, q_ref, g_ref, r_ref, x_ref = held
    problems, sections, nu, nx = b_ref.shape
    cols = sections * nu
    for p in range(problems):
        controls = b_ref[p].reshape(cols, nx).T
        drift = f_ref[p].T
        target = g_ref[p].T
        pad = jnp.zeros((nx, LANES - nx - 1), jnp.float32)
        section = iota((nx, cols), 1) // nu
        start = [
            jnp.concatenate(
                [
                    jnp.where(section == s, controls, 0.0),
                    jnp.concatenate([a_ref[p, s], drift[:, s : s + 1], pad], 1),
                ],
                1,
            )
            for s in range(sections)
        ]
        states = respond(0, sections, start)
        lane = iota((nx, cols + LANES), 1)
        errors = [
            jnp.where(lane == cols + nx, x - target[:, s : s + 1], x)
            for s, x in enumerate(states)
        ]
        weighted = [product(q_ref[p, s], e) for s, e in enumerate(errors)]
        square = product(jnp.concatenate(errors, 0), jnp.concatenate(weighted, 0), "tn")
        costs = r_ref[p].reshape(cols, nu)
        copies = (iota((nu, cols), 1) % nu == iota((nu, cols), 0)).astype(jnp.float32)
        same = iota((cols, cols), 0) // nu == iota((cols, cols), 1) // nu
        own_ref[p] = square[:cols, :cols] + jnp.where(same, product(costs, copies), 0.0)
        side_ref[p] = square[:cols, cols : cols + LANES]
        ones = jnp.ones((1, 1), jnp.float32)
        pad = jnp.zeros((1, LANES - nx - 1), jnp.float32)
        state_ref[p] = jnp.concatenate([x_ref[pl.ds(p, 1), :], ones, pad], 1)
        end = states[-1]
        pay_ref[p, :, :cols] = end[:, :cols]
        pay_ref[p, :, cols : cols + LANES] = jnp.concatenate(
            [end[:, cols : cols + HALF], square[cols : cols + nx, cols : cols + HALF]], 1
        )
        pay_ref[p, :, cols + LANES :] = square[cols : cols + nx, :cols]


def join_kernel(outer, inner, *refs):
    count = outer * inner
    pays, (own_ref, side_ref, x_ref, h_ref, grad_ref) = refs[:count], refs[count:]
    nx = pays[0].shape[1]
    device = lax.axis_index("horizon")
    place = lax.rem(device, inner)
    problems, cols, _ = own_ref.shape
    upper = [device + k < count for k in range(count)]
    for p in range(problems):

        def block(k):
            step, turn = k // inner, k % inner
            here = pays[step * inner + turn][p]
            if not turn:
                return here
            return jnp.where(
                place + turn >= inner, pays[(step + 1) % outer * inner + turn][p], here
            )

        blocks = [block(k) for k in range(count)]
        last = lambda x: jnp.where(iota(x.shape, 1) == nx, x, 0.0)
        moved = [None, blocks[0][:, :cols].T]
        sent = [None]
        for k in range(1, count):
            moved[k] = jnp.where(upper[k], moved[k], 0.0)
            sent.append(product(moved[k], blocks[k][:, cols:]))
            if k + 1 < count:
                moved.append(product(moved[k], blocks[k][:, cols : cols + nx], "nt"))
        carried = blocks[-1][:, cols : cols + HALF]
        entry = [None] * count
        entry[-1] = blocks[-1][:, :cols]
        eye = (iota((nx, HALF), 0) == iota((nx, HALF), 1)).astype(jnp.float32)
        carried = jnp.where(upper[-1], eye, carried)
        for k in reversed(range(1, count - 1)):
            step = product(carried[:, :nx], blocks[k][:, : cols + LANES])
            entry[k] = step[:, :cols]
            carried = jnp.where(
                upper[k], carried, step[:, cols : cols + HALF] + last(carried)
            )
        costate = sent[-1][:, HALF:LANES]
        tiles = [None] * count
        tiles[-1] = sent[-1][:, LANES:]
        for k in reversed(range(count - 1)):
            back = product(costate[:, :nx], blocks[k][:, : cols + LANES])
            if k:
                tiles[k] = sent[k][:, LANES:] + back[:, :cols]
                more = sent[k][:, HALF:LANES]
            else:
                tiles[k] = own_ref[p] + back[:, :cols]
                more = side_ref[p, :, :HALF]
            costate = back[:, cols : cols + HALF] + more + last(costate)
        for k in range(count):
            tile = tiles[k]
            if k:
                tile = jnp.where(upper[k], tile, product(costate[:, :nx], entry[k]))
            at = pl.multiple_of(lax.rem(device + k, count) * cols, cols)
            h_ref[p, :, pl.ds(at, cols)] = tile
        ones = jnp.ones((1, 1), jnp.float32)
        pad = jnp.zeros((1, HALF - nx - 1), jnp.float32)
        state = product(x_ref[p, :, :HALF], carried, "nt")
        state = jnp.concatenate([state, ones, pad], 1)
        grad_ref[pl.ds(p, 1), :] = product(state, costate, "nt")


def gather(block, count, inner):
    outer = count // inner
    sets = [[block]]
    for i in range(1, outer):
        pairs = [((d + i * inner) % count, d) for d in range(count)]
        sets.append([lax.ppermute(block, "horizon", pairs)])
    for group in sets:
        for j in range(1, inner):
            pairs = [(d // inner * inner + (d + j) % inner, d) for d in range(count)]
            group.append(lax.ppermute(group[0], "horizon", pairs))
    return [block for group in sets for block in group]


def body(dynamics, inputs, state_cost, input_cost, drift, target, initial):
    count = lax.axis_size("horizon")
    inner = 1
    while inner * inner * 4 <= count and count % (inner * 2) == 0:
        inner *= 2
    problems, sections, nx, nu = inputs.shape
    cols = sections * nu
    f32 = jnp.float32
    turned = jnp.swapaxes(inputs, 2, 3)
    operands = (dynamics, turned, drift, state_cost, target, input_cost, initial)
    operands = [pltpu.with_memory_space_constraint(x, pltpu.HBM) for x in operands]
    pay, own, side, state = pl.pallas_call(
        local_kernel,
        out_shape=(
            jax.ShapeDtypeStruct((problems, nx, 2 * cols + LANES), f32),
            jax.ShapeDtypeStruct((problems, cols, cols), f32),
            jax.ShapeDtypeStruct((problems, cols, LANES), f32),
            jax.ShapeDtypeStruct((problems, 1, LANES), f32),
        ),
        in_specs=[pl.BlockSpec(memory_space=pltpu.HBM)] * len(operands),
        scratch_shapes=[pltpu.VMEM(x.shape, x.dtype) for x in operands]
        + [pltpu.SemaphoreType.DMA((len(operands),))],
        compiler_params=pltpu.CompilerParams(vmem_limit_bytes=16 << 20),
        name="local",
    )(*operands)
    pays = gather(pay, count, inner)
    return pl.pallas_call(
        functools.partial(join_kernel, count // inner, inner),
        out_shape=(
            jax.ShapeDtypeStruct((problems, cols, count * cols), f32),
            jax.ShapeDtypeStruct((problems, cols), f32),
        ),
        compiler_params=pltpu.CompilerParams(vmem_limit_bytes=16 << 20),
        name="join",
    )(*pays, own, side, state)


def solution(mesh):
    in_specs = (
        P("batch", "horizon", None, None),
        P("batch", "horizon", None, None),
        P("batch", "horizon", None, None),
        P("batch", "horizon", None, None),
        P("batch", "horizon", None),
        P("batch", "horizon", None),
        P("batch", None),
    )
    out_specs = (P("batch", "horizon", None), P("batch", "horizon"))
    return jax.shard_map(body, mesh=mesh, in_specs=in_specs, out_specs=out_specs, check_vma=False)
```
